32 devices in a mesh: row: 8 (over z, y), col: 4 (over x, core).
Axes of the slice: x: 2, y: 2, z: 4, core: 2. Of those that a mesh axis runs over, the one named last changes fastest.
Arguments:
- weights: float32 [2, 4, 2048, 8, 1024], P(None, None, 'row', None, 'col'), may hold values from -6 to 6
Outputs:
- trailing: float32 [2, 4, 2048, 8, 1024], P(None, None, 'row', None, 'col')
- diagonal: float32 [2, 12], replicated
- superdiag: float32 [2, 12], replicated
The draws below stay inside these ranges and needn't reach their ends.
All inputs are finite; a program needn't handle non-finite values.
Results may differ from the reference program's by a relative error of at most 0.0003.
Values sent between devices are 32-bit elements; how exact they have to be, the bound alone decides.
A program may use at most 128 MiB of HBM per device.

```python
import jax
import jax.numpy as jnp
from jax import lax

N = 8192
TILE = 256
STEPS = 6
PANELS = 2
MATS = 2
RCYC = 4
CCYC = 8
N_ROW = 8
N_COL = 4


def level_of(rng, shape, split, low, top_value):
    loudness = 1.0
    for position, shards_of in split:
        draws = jax.random.uniform(jax.random.fold_in(jax.random.fold_in(rng, 6), position), (shards_of,), jnp.float32, low / len(split), top_value / len(split))
        loudness = loudness * jnp.repeat(jnp.exp(draws), shape[position] // shards_of).reshape((-1,) + (1,) * (len(shape) - 1 - position))
    return loudness


def scatter_about(own_key, dims, width, limit, pieces=(), kind=jnp.bfloat16):
    values = jax.random.normal(own_key, dims, jnp.float32) * width
    if len(pieces) > 0:
        values = level_of(own_key, dims, pieces, -0.22, 0.18) * values
    return jnp.clip(values, min=-limit, max=limit).astype(kind)


def setup_inputs(seed: int = 0) -> dict:
    key_list = jax.random.split(jax.random.key(seed), 2)
    return {
        "weights": scatter_about(key_list[0], (MATS, RCYC, N_ROW * TILE, CCYC, N_COL * TILE), 1.0, 6.0, ((2, 8), (4, 4)), jnp.float32),
    }


def contract(form, left, right):
    return jnp.einsum(form, left, right, precision=lax.Precision.HIGHEST)

def reflect(leading, squares):
    length = jnp.sqrt(squares)
    divisor = jnp.maximum(leading + length, 1.0)
    factor = (leading + length) / jnp.maximum(length, 1.0)
    return (divisor, factor, -length)

def reference(weights):
    mats = weights.reshape(MATS, N, N)
    global_ids = jnp.arange(N, dtype=jnp.int32)
    diag_list = []
    super_list = []
    for panel_at in range(PANELS):
        first_at = panel_at * STEPS
        col_refl = jnp.zeros((MATS, STEPS, N), jnp.float32)
        col_aux = jnp.zeros((MATS, STEPS, N), jnp.float32)
        row_aux = jnp.zeros((MATS, STEPS, N), jnp.float32)
        row_refl = jnp.zeros((MATS, STEPS, N), jnp.float32)
        for step_at in range(STEPS):
            pivot = first_at + step_at
            col_piece = mats[:, :, pivot] - contract('mp,mpr->mr', row_aux[:, :, pivot], col_refl) - contract('mp,mpr->mr', row_refl[:, :, pivot], col_aux)
            col_piece = jnp.where(global_ids >= pivot, col_piece, 0.0)
            divisor, factor, bidiag = reflect(col_piece[:, pivot], lax.optimization_barrier(jnp.sum(col_piece * col_piece, axis=1)))
            col_vec = jnp.where(global_ids == pivot, 1.0, col_piece / divisor[:, None])
            col_refl = col_refl.at[:, step_at].set(col_vec)
            weighs_one = contract('mpr,mr->mp', col_refl, col_vec)
            weighs_two = contract('mpr,mr->mp', col_aux, col_vec)
            col_img = factor[:, None] * (contract('mrc,mr->mc', mats, col_vec) - contract('mp,mpc->mc', weighs_one, row_aux) - contract('mp,mpc->mc', weighs_two, row_refl))
            col_img = jnp.where(global_ids > pivot, col_img, 0.0)
            row_aux = row_aux.at[:, step_at].set(col_img)
            row_piece = mats[:, pivot, :] - contract('mp,mpc->mc', col_refl[:, :, pivot], row_aux) - contract('mp,mpc->mc', col_aux[:, :, pivot], row_refl)
            row_piece = jnp.where(global_ids > pivot, row_piece, 0.0)
            divisor2, factor2, bidiag2 = reflect(row_piece[:, pivot + 1], lax.optimization_barrier(jnp.sum(row_piece * row_piece, axis=1)))
            row_vec = jnp.where(global_ids == pivot + 1, 1.0, row_piece / divisor2[:, None])
            row_refl = row_refl.at[:, step_at].set(row_vec)
            dots_one = contract('mpc,mc->mp', row_aux, row_vec)
            dots_two = contract('mpc,mc->mp', row_refl, row_vec)
            row_img = factor2[:, None] * (contract('mrc,mc->mr', mats, row_vec) - contract('mp,mpr->mr', dots_one, col_refl) - contract('mp,mpr->mr', dots_two, col_aux))
            row_img = jnp.where(global_ids > pivot, row_img, 0.0)
            col_aux = col_aux.at[:, step_at].set(row_img)
            diag_list.append(bidiag)
            super_list.append(bidiag2)
        mats = mats - contract('mpr,mpc->mrc', col_refl, row_aux) - contract('mpr,mpc->mrc', col_aux, row_refl)
    done = PANELS * STEPS
    inside = (global_ids[:, None] >= done) & (global_ids[None, :] >= done)
    trailing = jnp.where(inside[None], mats, 0.0).reshape(weights.shape)
    return (trailing, jnp.stack(diag_list, axis=1), jnp.stack(super_list, axis=1))
```

```python
import functools

import jax
import jax.numpy as jnp
from jax import lax
from jax.experimental import pallas as pl
from jax.experimental.pallas import tpu as pltpu
from jax.sharding import PartitionSpec as P

STEPS = 6
PANELS = 2
TOTAL = STEPS * PANELS
SLOTS = 16
LANES = 128
MESH = pl.DeviceIdType.MESH


def reflect(leading, squares):
    length = jnp.sqrt(squares)
    divisor = jnp.maximum(leading + length, 1.0)
    factor = (leading + length) / jnp.maximum(length, 1.0)
    return (divisor, factor, -length)


def peers(axis, count):
    me = lax.axis_index(axis)
    return [(lax.rem(me + d, count), lax.rem(me - d + count, count)) for d in range(1, count)]


def positions(length, tile_len, devices, place):
    ids = lax.broadcasted_iota(jnp.int32, (1, length), 1)
    return ids // tile_len * (devices * tile_len) + place * tile_len + ids % tile_len


def pack(batch):
    lane = lax.broadcasted_iota(jnp.int32, (8, LANES), 1)
    tile = jnp.zeros((8, LANES), jnp.float32)
    groups = 2 * SLOTS // 8
    at = 0
    for dots, picked, squares, leading in batch:
        for column in (dots, picked):
            for g in range(groups):
                tile = jnp.where(lane == at, column[g * 8 : (g + 1) * 8], tile)
                at += 1
        for scalar in (squares, leading):
            tile = jnp.where(lane == at, scalar, tile)
            at += 1
    return tile


def unpack(tile, batch_n):
    groups = 2 * SLOTS // 8
    at = 0
    result = []
    for _ in range(batch_n):
        columns = []
        for _ in range(2):
            columns.append(
                jnp.concatenate([tile[:, at + g : at + g + 1] for g in range(groups)], axis=0)
            )
            at += groups
        result.append((columns[0], columns[1], tile[0:1, at : at + 1], tile[0:1, at + 1 : at + 2]))
        at += 2
    return result


def exchange(axis, count, par, big, small, sems):
    send_sem, recv_sem = sems
    me = lax.axis_index(axis)

    def copies(source, target, at):
        return [
            pltpu.make_async_remote_copy(
                src_ref=ref.at[par, source],
                dst_ref=ref.at[par, source],
                send_sem=send_sem.at[which, at],
                recv_sem=recv_sem.at[par, which, source],
                device_id={axis: target},
                device_id_type=MESH,
            )
            for which, ref in enumerate((big, small))
        ]

    sends = []
    for at, (to, _) in enumerate(peers(axis, count)):
        for copy in copies(me, to, at):
            copy.start()
            sends.append(copy)
    for at, (_, source) in enumerate(peers(axis, count)):
        for copy in copies(source, source, at):
            copy.wait_recv()
    for copy in sends:
        copy.wait_send()


def kernel(
    row_n, col_n, tile_len, mats, vx, yu, bid,
    cols, rows, spread, sums, row_big, row_small, col_big, col_small,
    row_send, row_recv, col_send, col_recv, slab_send, slab_recv,
):
    batch_n, height, width = mats.shape
    row_place = lax.axis_index("row")
    col_place = lax.axis_index("col")
    barrier = pltpu.get_barrier_semaphore()
    for axis, count in (("row", row_n), ("col", col_n)):
        for to, _ in peers(axis, count):
            pl.semaphore_signal(barrier, inc=1, device_id={axis: to}, device_id_type=MESH)
    pl.semaphore_wait(barrier, row_n + col_n - 2)

    def slab_copy(ref, axis, which, to, at):
        return pltpu.make_async_remote_copy(
            src_ref=ref,
            dst_ref=ref,
            send_sem=slab_send.at[which, at],
            recv_sem=slab_recv.at[which],
            device_id={axis: to},
            device_id_type=MESH,
        )

    slabs = (("col", col_n, cols, col_place), ("row", row_n, rows, row_place))

    @pl.when(col_place == 0)
    def _():
        for m in range(batch_n):
            for b in range(height // LANES):
                span = pl.ds(b * LANES, LANES)
                cols[m, :, span] = mats[m, span, 0:LANES].T[0:SLOTS]
        for at in range(1, col_n):
            slab_copy(cols, "col", 0, at, at).start()

    @pl.when(row_place == 0)
    def _():
        for m in range(batch_n):
            rows[m] = mats[m, 0:SLOTS, :]
        for at in range(1, row_n):
            slab_copy(rows, "row", 1, at, at).start()

    vx[...] = jnp.zeros_like(vx)
    yu[...] = jnp.zeros_like(yu)
    bid[...] = jnp.zeros_like(bid)

    @pl.when(col_place != 0)
    def _():
        slab_copy(cols, "col", 0, 0, 0).wait_recv()

    grow = positions(height, tile_len, row_n, row_place)
    gcol = positions(width, tile_len, col_n, col_place)
    slot = lax.broadcasted_iota(jnp.int32, (2 * SLOTS, 1), 0)
    lane = lax.broadcasted_iota(jnp.int32, (1, LANES), 1)
    own_row = jnp.where(row_place == 0, lane, -1)
    own_col = jnp.where(col_place == 0, lane, -1)
    row_at = lax.broadcasted_iota(jnp.int32, (8, LANES), 0)
    lane_at = lax.broadcasted_iota(jnp.int32, (8, LANES), 1)

    def full_sum(value):
        return jnp.sum(value, axis=1, keepdims=True)

    def step_body(step, weighs):
        par = lax.rem(step, 2)
        col_pieces = []
        batch = []
        for m in range(batch_n):
            old = vx[m]
            piece = cols[m, pl.ds(step, 1), :] - jnp.sum(weighs[m] * old, axis=0, keepdims=True)
            piece = jnp.where(grow >= step, piece, 0.0)
            batch.append(
                (
                    full_sum(old * piece),
                    full_sum(jnp.where(own_row == step, old[:, 0:LANES], 0.0)),
                    full_sum(piece * piece),
                    full_sum(jnp.where(grow == step, piece, 0.0)),
                )
            )
            col_pieces.append(piece)
            for b in range(height // LANES):
                span = slice(b * LANES, (b + 1) * LANES)
                spread[m, span, :] = jnp.broadcast_to(piece[:, span], (LANES, LANES)).T
        for m in range(batch_n):

            def add_rows(at, total):
                span = pl.ds(pl.multiple_of(at * 8, 8), 8)
                scale = spread[m, span, :]
                return tuple(
                    total[t] + mats[m, span, t * LANES : (t + 1) * LANES] * scale
                    for t in range(width // LANES)
                )

            zeros = tuple(jnp.zeros((8, LANES), jnp.float32) for _ in range(width // LANES))
            total = lax.fori_loop(0, height // 8, add_rows, zeros, unroll=4)
            row_big[par, row_place, m : m + 1, :] = jnp.concatenate(
                [jnp.sum(t, axis=0, keepdims=True) for t in total], axis=1
            )
        row_small[par, row_place] = pack(batch)
        exchange("row", row_n, par, row_big, row_small, (row_send, row_recv))

        @pl.when((row_place != 0) & (step == 0))
        def _():
            slab_copy(rows, "row", 1, 0, 0).wait_recv()

        small = row_small[par, 0]
        trans = row_big[par, 0]
        for s in range(1, row_n):
            small = small + row_small[par, s]
            trans = trans + row_big[par, s]
        small_list = unpack(small, batch_n)
        row_pieces = []
        batch = []
        marks = bid[...]
        for m in range(batch_n):
            dots, picked, squares, leading = small_list[m]
            divisor, factor, bidiag = reflect(leading, squares)
            marks = jnp.where((row_at == m) & (lane_at == step), bidiag, marks)
            remain = 1.0 - leading / divisor
            vx[m, pl.ds(step, 1), :] = jnp.where(grow == step, 1.0, col_pieces[m] / divisor)
            pivot_row = rows[m, pl.ds(step, 1), :]
            old = yu[m]
            weight = dots / divisor + picked * remain
            image = factor * (
                trans[m : m + 1] / divisor
                + pivot_row * remain
                - jnp.sum(weight * old, axis=0, keepdims=True)
            )
            image = jnp.where(gcol > step, image, 0.0)
            yu[m, pl.ds(step, 1), :] = image
            piece = pivot_row - image - jnp.sum(picked * old, axis=0, keepdims=True)
            piece = jnp.where(gcol > step, piece, 0.0)
            new = yu[m]
            batch.append(
                (
                    full_sum(new * piece),
                    full_sum(jnp.where(own_col == step + 1, new[:, 0:LANES], 0.0)),
                    full_sum(piece * piece),
                    full_sum(jnp.where(gcol == step + 1, piece, 0.0)),
                )
            )
            row_pieces.append(piece)
        for m in range(batch_n):
            piece = row_pieces[m]
            scale = [
                jnp.broadcast_to(piece[:, t * LANES : (t + 1) * LANES], (8, LANES))
                for t in range(width // LANES)
            ]

            @pl.loop(0, height // 8, unroll=4)
            def _(at):
                span = pl.ds(pl.multiple_of(at * 8, 8), 8)
                parts = [
                    mats[m, span, t * LANES : (t + 1) * LANES] * scale[t]
                    for t in range(width // LANES)
                ]
                while len(parts) > 1:
                    parts = [
                        parts[i] + parts[i + 1] if i + 1 < len(parts) else parts[i]
                        for i in range(0, len(parts), 2)
                    ]
                sums[m, span, :] = parts[0]

        for m in range(batch_n):
            for b in range(height // LANES):
                span = slice(b * LANES, (b + 1) * LANES)
                col_big[par, col_place, m : m + 1, span] = jnp.sum(
                    sums[m, span, :].T, axis=0, keepdims=True
                )
        col_small[par, col_place] = pack(batch)
        exchange("col", col_n, par, col_big, col_small, (col_send, col_recv))
        small = col_small[par, 0]
        applied = col_big[par, 0]
        for s in range(1, col_n):
            small = small + col_small[par, s]
            applied = applied + col_big[par, s]
        small_list = unpack(small, batch_n)
        later = []
        for m in range(batch_n):
            dots, picked, squares, leading = small_list[m]
            divisor, factor, bidiag = reflect(leading, squares)
            marks = jnp.where((row_at == m) & (lane_at == step + SLOTS), bidiag, marks)
            remain = 1.0 - leading / divisor
            yu[m, pl.ds(SLOTS + step, 1), :] = jnp.where(
                gcol == step + 1, 1.0, row_pieces[m] / divisor
            )
            weight = dots / divisor + picked * remain
            image = factor * (
                applied[m : m + 1] / divisor
                + cols[m, pl.ds(step + 1, 1), :] * remain
                - jnp.sum(weight * vx[m], axis=0, keepdims=True)
            )
            vx[m, pl.ds(SLOTS + step, 1), :] = jnp.where(grow > step, image, 0.0)
            later.append(jnp.where(slot == SLOTS + step, 1.0, picked))
        bid[...] = marks
        return tuple(later)

    none = tuple(jnp.zeros((2 * SLOTS, 1), jnp.float32) for _ in range(batch_n))
    lax.fori_loop(0, TOTAL, step_body, none)

    for which, (axis, count, ref, place) in enumerate(slabs):

        @pl.when(place == 0)
        def _():
            for at in range(1, count):
                slab_copy(ref, axis, which, at, at).wait_send()


def factor_all(mats, row_n, col_n, tile_len):
    batch_n, height, width = mats.shape
    whole = pl.BlockSpec(memory_space=pltpu.VMEM)
    f32 = jnp.float32
    return pl.pallas_call(
        functools.partial(kernel, row_n, col_n, tile_len),
        out_shape=(
            jax.ShapeDtypeStruct((batch_n, 2 * SLOTS, height), f32),
            jax.ShapeDtypeStruct((batch_n, 2 * SLOTS, width), f32),
            jax.ShapeDtypeStruct((8, LANES), f32),
        ),
        in_specs=[whole],
        out_specs=(whole, whole, whole),
        scratch_shapes=[
            pltpu.VMEM((batch_n, SLOTS, height), f32),
            pltpu.VMEM((batch_n, SLOTS, width), f32),
            pltpu.VMEM((batch_n, height, LANES), f32),
            pltpu.VMEM((batch_n, height, LANES), f32),
            pltpu.VMEM((2, row_n, batch_n, width), f32),
            pltpu.VMEM((2, row_n, 8, LANES), f32),
            pltpu.VMEM((2, col_n, batch_n, height), f32),
            pltpu.VMEM((2, col_n, 8, LANES), f32),
            pltpu.SemaphoreType.DMA((2, row_n)),
            pltpu.SemaphoreType.DMA((2, 2, row_n)),
            pltpu.SemaphoreType.DMA((2, col_n)),
            pltpu.SemaphoreType.DMA((2, 2, col_n)),
            pltpu.SemaphoreType.DMA((2, max(row_n, col_n))),
            pltpu.SemaphoreType.DMA((2,)),
        ],
        compiler_params=pltpu.CompilerParams(
            collective_id=0, has_side_effects=True, vmem_limit_bytes=48 * 1024 * 1024
        ),
    )(mats)


def per_device(weights):
    batch_n, row_cycles, tile_len, col_cycles, _ = weights.shape
    height = row_cycles * tile_len
    width = col_cycles * tile_len
    row_n = lax.axis_size("row")
    col_n = lax.axis_size("col")
    mats = weights.reshape(batch_n, height, width)
    vx, yu, bid = factor_all(mats, row_n, col_n, tile_len)
    grow = positions(height, tile_len, row_n, lax.axis_index("row"))[0]
    gcol = positions(width, tile_len, col_n, lax.axis_index("col"))[0]
    inside = (grow[:, None] >= TOTAL) & (gcol[None, :] >= TOTAL)
    update = jnp.einsum("mpr,mpc->mrc", vx, yu, precision=lax.Precision.HIGH)
    trailing = jnp.where(inside[None], mats - update, 0.0).reshape(weights.shape)
    return (trailing, bid[:batch_n, :TOTAL], bid[:batch_n, SLOTS : SLOTS + TOTAL])


def solution(mesh):
    placed = (P(None, None, "row", None, "col"),)
    return jax.shard_map(
        per_device,
        mesh=mesh,
        in_specs=placed,
        out_specs=(P(None, None, "row", None, "col"), P(), P()),
        check_vma=False,
    )
```
